32 devices in a mesh: dp: 4 (over x, core), row: 2 (over y), col: 4 (over z).
Axes of the slice: x: 2, y: 2, z: 4, core: 2. Of those that a mesh axis runs over, the one named last changes fastest.
Arguments:
- act_in: bfloat16 [4096, 2304], P(('dp', 'row'), 'col'), may hold values from -6 to 6
- cot_out: bfloat16 [4096, 2304], P(('dp', 'row'), 'col'), may hold values from -6 to 6
- w_gate: bfloat16 [2304, 4608], P(('dp', 'row'), 'col'), may hold values from -0.125 to 0.125
- w_up: bfloat16 [2304, 4608], P(('dp', 'row'), 'col'), may hold values from -0.125 to 0.125
- w_down: bfloat16 [4608, 2304], P('col', ('dp', 'row')), may hold values from -0.09375 to 0.09375
Outputs:
- input_grad: bfloat16 [4096, 2304], P(('dp', 'row'), 'col')
- gate_grad: float32 [2304, 4608], P(('dp', 'row'), 'col')
- up_grad: float32 [2304, 4608], P(('dp', 'row'), 'col')
- down_grad: float32 [4608, 2304], P('col', ('dp', 'row'))
The draws below stay inside these ranges and needn't reach their ends.
All inputs are finite; a program needn't handle non-finite values.
Results may differ from the reference program's by a relative error of at most 0.015.
Values may be sent and summed in bfloat16 or wider, within the bound.
No kernel may reach another device: no remote copies, remote signals or barrier semaphores. Data moves between devices by JAX's collectives and lax.ppermute only.
A program may use at most 128 MiB of HBM per device.

```python
import math
import jax
import jax.numpy as jnp
from jax import lax

D = 2304
FF = 4608
TOKENS = 4096
N_COL = 4


def with_spikes(result, key, source, target, shards_of, factor):
    def block_of(position):
        return (jnp.arange(result.shape[position]) // (result.shape[position] // shards_of)).reshape((-1,) + (1,) * (result.ndim - 1 - position))

    near = jax.random.permutation(key, shards_of)[block_of(target)]
    second = (block_of(target) + shards_of // 2) % shards_of
    return jnp.where((block_of(source) == near) | (block_of(source) == second), factor * result, result)


def levels(stream_key, dims, split, smallest, largest):
    loudness, own = 1.0, jax.random.fold_in(stream_key, 6)
    for dim, blocks in split:
        heights = jnp.exp(jax.random.uniform(jax.random.fold_in(own, dim), (blocks,), jnp.float32, smallest / len(split), largest / len(split)))
        loudness = loudness * jnp.repeat(heights, dims[dim] // blocks).reshape([-1 if axis == dim else 1 for axis in range(len(dims))])
    return loudness


def gaussian(rng, extent, deviation, reach, pieces=(), held_as=jnp.bfloat16):
    array = deviation * jax.random.normal(rng, extent, jnp.float32)
    if pieces:
        array = array * levels(rng, extent, pieces, -0.22, 0.18)
    return jnp.clip(array, -reach, reach).astype(held_as)


def heavy_noise(rng, extent, spread, bound, cuts, heavy, dtype=jnp.bfloat16):
    values = spread * jax.random.normal(rng, extent, jnp.float32)
    if cuts:
        values = values * levels(rng, extent, cuts, -0.22, 0.18)
    return jnp.clip(with_spikes(values, jax.random.fold_in(rng, 3), *heavy), -bound, bound).astype(dtype)


def setup_inputs(seed: int = 0) -> dict:
    splits = jax.random.split(jax.random.key(seed), 6)
    act_in = heavy_noise(splits[0], (TOKENS, D), 1.0, 6.0, ((0, 8), (1, 4)), (0, 1, 8, 2.0))
    cot_out = heavy_noise(splits[1], (TOKENS, D), 1.0, 6.0, ((0, 8), (1, 4)), (0, 1, 8, 2.0))
    w_gate = gaussian(splits[2], (D, FF), D ** -0.5, 0.125, ((0, 8), (1, 4)))
    w_up = gaussian(splits[3], (D, FF), D ** -0.5, 0.125, ((0, 8), (1, 4)))
    w_down = gaussian(splits[4], (FF, D), FF ** -0.5, 0.09375, ((0, 4), (1, 8)))
    return {"act_in": act_in, "cot_out": cot_out, "w_gate": w_gate, "w_up": w_up, "w_down": w_down}


gelu_cubic = 0.044715
gelu_scale = 0.7978845608028654

def gelu_parts(values):
    inner_arg = gelu_scale * (values + gelu_cubic * values * values * values)
    tanh_val = jnp.tanh(inner_arg)
    output = 0.5 * values * (1.0 + tanh_val)
    slope_val = 0.5 * (1.0 + tanh_val) + 0.5 * values * (1.0 - tanh_val * tanh_val) * gelu_scale * (1.0 + 3.0 * gelu_cubic * values * values)
    return (output, slope_val)

def reference(act_in, cot_out, w_gate, w_up, w_down):
    gate_pre = jnp.dot(act_in, w_gate, preferred_element_type=jnp.float32)
    up_pre = jnp.dot(act_in, w_up, preferred_element_type=jnp.float32)
    act_val, slope_val = gelu_parts(gate_pre)
    hidden = (act_val * up_pre).astype(jnp.bfloat16)
    hidden_grad = jnp.dot(cot_out, w_down.T, preferred_element_type=jnp.float32)
    d_gate = (hidden_grad * up_pre * slope_val).astype(jnp.bfloat16)
    d_up = (hidden_grad * act_val).astype(jnp.bfloat16)
    width = FF // N_COL
    input_sum = jnp.zeros(act_in.shape, jnp.float32)
    for column in range(N_COL):
        low_edge = column * width
        part_sum = jnp.dot(d_gate[:, low_edge:low_edge + width], w_gate[:, low_edge:low_edge + width].T, preferred_element_type=jnp.float32)
        part_sum = part_sum + jnp.dot(d_up[:, low_edge:low_edge + width], w_up[:, low_edge:low_edge + width].T, preferred_element_type=jnp.float32)
        input_sum = input_sum + lax.optimization_barrier(part_sum.astype(jnp.bfloat16)).astype(jnp.float32)
    input_grad = input_sum.astype(jnp.bfloat16)
    norm_scale = 1.0 / math.sqrt(TOKENS)
    gate_grad = jnp.dot(act_in.T, d_gate, preferred_element_type=jnp.float32) * norm_scale
    up_grad = jnp.dot(act_in.T, d_up, preferred_element_type=jnp.float32) * norm_scale
    down_grad = jnp.dot(hidden.T, cot_out, preferred_element_type=jnp.float32) * norm_scale
    return (input_grad, gate_grad, up_grad, down_grad)
```

```python
import math

import jax
import jax.numpy as jnp
from jax import lax
from jax.sharding import PartitionSpec as P


gelu_cubic = 0.044715
gelu_scale = 0.7978845608028654
GROUP = ("dp", "row")
FAR, NEAR, ROW = 4, 2, 1
OWN_MASKS = (0, ROW, FAR, FAR | ROW)
MASKS = OWN_MASKS + tuple(m | NEAR for m in OWN_MASKS)


def gelu_parts(values):
    inner_arg = gelu_scale * (values + gelu_cubic * values * values * values)
    tanh_val = jnp.tanh(inner_arg)
    output = 0.5 * values * (1.0 + tanh_val)
    slope_val = 0.5 * (1.0 + tanh_val) + 0.5 * values * (1.0 - tanh_val * tanh_val) * gelu_scale * (
        1.0 + 3.0 * gelu_cubic * values * values
    )
    return (output, slope_val)


def token_contract(left, right):
    return lax.dot_general(
        left, right, (((0,), (0,)), ((), ())), preferred_element_type=jnp.float32
    )


def plain_body(act_in, cot_out, w_gate, w_up, w_down):
    tok_rows = act_in.shape[0]
    act_full = lax.all_gather(act_in, "col", axis=1, tiled=True)
    cot_full = lax.all_gather(cot_out, "col", axis=1, tiled=True)
    gate_cols = lax.all_gather(w_gate, GROUP, axis=0, tiled=True)
    up_cols = lax.all_gather(w_up, GROUP, axis=0, tiled=True)
    down_rows = lax.all_gather(w_down, GROUP, axis=1, tiled=True)
    gate_pre = jnp.dot(act_full, gate_cols, preferred_element_type=jnp.float32)
    up_pre = jnp.dot(act_full, up_cols, preferred_element_type=jnp.float32)
    feature_dims = (((1,), (1,)), ((), ()))
    hidden_grad = lax.dot_general(
        cot_full, down_rows, feature_dims, preferred_element_type=jnp.float32
    )
    act_val, slope_val = gelu_parts(gate_pre)
    hidden = (act_val * up_pre).astype(jnp.bfloat16)
    d_gate = (hidden_grad * up_pre * slope_val).astype(jnp.bfloat16)
    d_up = (hidden_grad * act_val).astype(jnp.bfloat16)
    part_sum = lax.dot_general(d_gate, gate_cols, feature_dims, preferred_element_type=jnp.float32)
    part_sum = part_sum + lax.dot_general(
        d_up, up_cols, feature_dims, preferred_element_type=jnp.float32
    )
    input_grad = lax.psum_scatter(
        part_sum.astype(jnp.bfloat16), "col", scatter_dimension=1, tiled=True
    )
    norm_scale = 1.0 / math.sqrt(tok_rows * lax.axis_size(GROUP))

    def scattered(left, right):
        share = lax.psum_scatter(
            token_contract(left, right).astype(jnp.bfloat16),
            GROUP,
            scatter_dimension=0,
            tiled=True,
        )
        return share.astype(jnp.float32) * norm_scale

    return (
        input_grad,
        scattered(act_full, d_gate),
        scattered(act_full, d_up),
        scattered(cot_full, hidden).T,
    )


def hop(value, mask, size):
    return lax.ppermute(value, GROUP, [(i, i ^ mask) for i in range(size)])


def line_gather(own, n_col):
    place = lax.axis_index("col")
    ups, downs = [own], [own]
    for step in range(1, n_col):
        ups.append(lax.ppermute(ups[-1], "col", [(i, i + 1) for i in range(step - 1, n_col - 1)]))
        downs.append(lax.ppermute(downs[-1], "col", [(i, i - 1) for i in range(1, n_col - step + 1)]))
    pieces = [own]
    for step in range(1, n_col):
        pieces.append(jnp.where(place + step < n_col, downs[step], ups[n_col - step]))
    return jnp.stack(pieces)


def gather_weight(own, size):
    half = own.shape[0] // 2
    by_far, by_row = hop(own, FAR, size), hop(own, ROW, size)
    corner_top = hop(by_far[:half], ROW, size)
    corner_low = hop(by_row[half:], FAR, size)
    mine = [own, by_row, by_far, corner_top, corner_low]
    return jnp.concatenate(mine + [hop(v, NEAR, size) for v in mine], axis=0)


def scatter_weight(partial_of, size):
    other = hop(partial_of(True), NEAR, size)
    total = partial_of(False) + other
    half = total.shape[1] // 2
    top, low = total[:, :half], total[:, half:]
    from_far = hop(jnp.stack([top[2], top[3]]), FAR, size)
    from_row = hop(jnp.stack([low[1], low[3]]), ROW, size)
    top_own = top[0] + from_far[0]
    low_own = low[0] + from_row[0]
    top_last = hop(top[1] + from_far[1], ROW, size)
    low_last = hop(low[2] + from_row[1], FAR, size)
    f32 = jnp.float32
    return jnp.concatenate(
        [
            top_own.astype(f32) + top_last.astype(f32),
            low_own.astype(f32) + low_last.astype(f32),
        ],
        axis=0,
    )


def line_scatter(blocks_of, n_col):
    place = lax.axis_index("col")
    down = up = None
    for step in range(1, n_col):
        low = blocks_of(jnp.clip(step + place - n_col, 0, n_col - 1))
        high = blocks_of(jnp.clip(place + n_col - step, 0, n_col - 1))
        if down is not None:
            low, high = low + down, high + up
        down = lax.ppermute(low, "col", [(i, i - 1) for i in range(n_col - step, n_col)])
        up = lax.ppermute(high, "col", [(i, i + 1) for i in range(0, step)])
    f32 = jnp.float32
    return (blocks_of(place).astype(f32) + down.astype(f32) + up.astype(f32)).astype(jnp.bfloat16)


def hop_body(size, n_col, act_in, cot_out, w_gate, w_up, w_down):
    tok_rows = act_in.shape[0]
    rows = w_gate.shape[0]
    me = lax.axis_index(GROUP)
    place = lax.axis_index("col")
    per_col = size // n_col

    def in_mask_order(pieces):
        flat = pieces.reshape((size, rows, tok_rows))
        out = []
        for mask in MASKS:
            k = me ^ mask
            at = lax.rem(k // per_col - place + n_col, n_col) * per_col + lax.rem(k, per_col)
            out.append(lax.dynamic_index_in_dim(flat, at, 0, keepdims=False))
        return jnp.concatenate(out, axis=0)

    act_t = in_mask_order(line_gather(act_in.T, n_col))
    gate_rows = gather_weight(w_gate, size)
    up_rows = gather_weight(w_up, size)
    cot_t = in_mask_order(line_gather(cot_out.T, n_col))
    down_rows = gather_weight(w_down.T, size)

    gate_pre = token_contract(act_t, gate_rows)
    up_pre = token_contract(act_t, up_rows)
    act_val, slope_val = gelu_parts(gate_pre)
    hidden = (act_val * up_pre).astype(jnp.bfloat16)
    hidden_grad = token_contract(cot_t, down_rows)
    d_gate = (hidden_grad * up_pre * slope_val).astype(jnp.bfloat16)
    d_up = (hidden_grad * act_val).astype(jnp.bfloat16)

    norm_scale = 1.0 / math.sqrt(tok_rows * size)
    own_rows = rows * len(OWN_MASKS)

    def weight_grad(left_t, right):
        def partial_of(near):
            part = left_t[own_rows:] if near else left_t[:own_rows]
            out = jnp.dot(part, right, preferred_element_type=jnp.float32).astype(jnp.bfloat16)
            return out.reshape((len(OWN_MASKS), rows, -1))

        return scatter_weight(partial_of, size) * norm_scale

    down_grad = weight_grad(cot_t, hidden).T
    gate_grad = weight_grad(act_t, d_gate)
    up_grad = weight_grad(act_t, d_up)

    feature_dims = (((1,), (1,)), ((), ()))
    part_sum = lax.dot_general(gate_rows, d_gate, feature_dims, preferred_element_type=jnp.float32)
    part_sum = part_sum + lax.dot_general(
        up_rows, d_up, feature_dims, preferred_element_type=jnp.float32
    )
    blocks = part_sum.astype(jnp.bfloat16).reshape((size, rows, tok_rows))

    def blocks_of(s):
        out = []
        for b in range(per_col):
            mask = (s * per_col + b) ^ me
            at = (mask & NEAR) * 2 + (mask & FAR) // 2 + (mask & ROW)
            out.append(lax.dynamic_index_in_dim(blocks, at, 0, keepdims=False))
        return jnp.concatenate(out, axis=0)

    input_grad = line_scatter(blocks_of, n_col).T
    return (input_grad, gate_grad, up_grad, down_grad)


def solution(mesh):
    n_dp, n_row, n_col = (mesh.shape[a] for a in ("dp", "row", "col"))
    size = n_dp * n_row
    by_tokens = P(GROUP, "col")
    hops = size == len(MASKS) and n_row == 2 and size % n_col == 0

    def body(*args):
        return hop_body(size, n_col, *args) if hops else plain_body(*args)

    return jax.shard_map(
        body,
        mesh=mesh,
        in_specs=(by_tokens,) * 4 + (P("col", GROUP),),
        out_specs=(by_tokens,) * 3 + (P("col", GROUP),),
        check_vma=False,
    )
```

```python
import math

import jax
import jax.numpy as jnp
from jax import lax
from jax.experimental import pallas as pl
from jax.experimental.pallas import tpu as pltpu
from jax.sharding import PartitionSpec as P


gelu_cubic = 0.044715
gelu_scale = 0.7978845608028654
GROUP = ("dp", "row")
FAR, NEAR, ROW = 4, 2, 1
OWN_MASKS = (0, ROW, FAR, FAR | ROW)
MASKS = OWN_MASKS + tuple(m | NEAR for m in OWN_MASKS)


def gelu_parts(values):
    inner_arg = gelu_scale * (values + gelu_cubic * values * values * values)
    tanh_val = jnp.tanh(inner_arg)
    output = 0.5 * values * (1.0 + tanh_val)
    slope_val = 0.5 * (1.0 + tanh_val) + 0.5 * values * (1.0 - tanh_val * tanh_val) * gelu_scale * (
        1.0 + 3.0 * gelu_cubic * values * values
    )
    return (output, slope_val)


def token_contract(left, right):
    return lax.dot_general(
        left, right, (((0,), (0,)), ((), ())), preferred_element_type=jnp.float32
    )


def plain_body(act_in, cot_out, w_gate, w_up, w_down):
    tok_rows = act_in.shape[0]
    act_full = lax.all_gather(act_in, "col", axis=1, tiled=True)
    cot_full = lax.all_gather(cot_out, "col", axis=1, tiled=True)
    gate_cols = lax.all_gather(w_gate, GROUP, axis=0, tiled=True)
    up_cols = lax.all_gather(w_up, GROUP, axis=0, tiled=True)
    down_rows = lax.all_gather(w_down, GROUP, axis=1, tiled=True)
    gate_pre = jnp.dot(act_full, gate_cols, preferred_element_type=jnp.float32)
    up_pre = jnp.dot(act_full, up_cols, preferred_element_type=jnp.float32)
    feature_dims = (((1,), (1,)), ((), ()))
    hidden_grad = lax.dot_general(
        cot_full, down_rows, feature_dims, preferred_element_type=jnp.float32
    )
    act_val, slope_val = gelu_parts(gate_pre)
    hidden = (act_val * up_pre).astype(jnp.bfloat16)
    d_gate = (hidden_grad * up_pre * slope_val).astype(jnp.bfloat16)
    d_up = (hidden_grad * act_val).astype(jnp.bfloat16)
    part_sum = lax.dot_general(d_gate, gate_cols, feature_dims, preferred_element_type=jnp.float32)
    part_sum = part_sum + lax.dot_general(
        d_up, up_cols, feature_dims, preferred_element_type=jnp.float32
    )
    input_grad = lax.psum_scatter(
        part_sum.astype(jnp.bfloat16), "col", scatter_dimension=1, tiled=True
    )
    norm_scale = 1.0 / math.sqrt(tok_rows * lax.axis_size(GROUP))

    def scattered(left, right):
        share = lax.psum_scatter(
            token_contract(left, right).astype(jnp.bfloat16),
            GROUP,
            scatter_dimension=0,
            tiled=True,
        )
        return share.astype(jnp.float32) * norm_scale

    return (
        input_grad,
        scattered(act_full, d_gate),
        scattered(act_full, d_up),
        scattered(cot_full, hidden).T,
    )


def hop(value, mask, size):
    return lax.ppermute(value, GROUP, [(i, i ^ mask) for i in range(size)])


def shift(value, pairs):
    return lax.ppermute(value, "col", pairs)


def middle(value, size):
    pairs = []
    for i in range(size):
        for place, (to, mask) in enumerate(((0, NEAR), (2, 0), (1, 0), (3, NEAR))):
            pairs.append((i * 4 + place, (i ^ mask) * 4 + to))
    return lax.ppermute(value, (*GROUP, "col"), pairs)


def line_gather(own, size):
    outer = [(0, 1), (1, 0), (2, 3), (3, 2)]
    beside = shift(own, outer)
    over = middle(own, size)
    over_far = middle(beside, size)
    end = shift(over, outer)
    end_far = shift(over_far, outer)
    return [own, beside, over, end, over_far, end_far]


def line_slot(piece):
    place = lax.axis_index("col")
    at_end = ((place == 0) | (place == 3)).astype(jnp.int32)
    near_first = jnp.where(place < 2, piece == 2, piece == 1)
    other = jnp.where(near_first, 2, 4) + at_end
    return jnp.where(((place ^ piece) & 2) == 0, place ^ piece, other)


def fetch_rows(source, pieces, target, sems, places):
    rows = target.shape[0] // len(places)
    for at, place in enumerate(places):
        for i, piece in enumerate(pieces):

            @pl.when(source[0, place] == i)
            def _(piece=piece, at=at, place=place):
                first = pl.multiple_of(source[1, place] * rows, 16)
                pltpu.make_async_copy(
                    piece.at[pl.ds(first, rows)], target.at[pl.ds(at * rows, rows)], sems.at[at]
                ).start()

    def wait(at):
        pltpu.make_async_copy(
            pieces[0].at[pl.ds(0, rows)], target.at[pl.ds(at * rows, rows)], sems.at[at]
        ).wait()

    return wait


def fetch_pieces(pieces, target, sems):
    copies, at = [], 0
    for i, piece in enumerate(pieces):
        rows = piece.shape[0]
        copies.append(pltpu.make_async_copy(piece, target.at[pl.ds(at, rows)], sems.at[i]))
        copies[-1].start()
        at += rows
    return copies


def rows_kernel(source, *refs):
    pieces, (out, sems) = refs[:6], refs[6:]
    wait = fetch_rows(source, pieces, out, sems, range(len(MASKS)))
    for at in range(len(MASKS)):
        wait(at)


def pieces_kernel(*refs):
    pieces, (out, sems) = refs[:-2], refs[-2:]
    for copy in fetch_pieces(pieces, out, sems):
        copy.wait()


def lay_out(pieces, shape, source=None):
    n_sems = len(MASKS) if source is not None else len(pieces)
    table = [] if source is None else [source]
    in_hbm = [pl.BlockSpec(memory_space=pltpu.HBM)] * len(pieces)
    return pl.pallas_call(
        pieces_kernel if source is None else rows_kernel,
        in_specs=[pl.BlockSpec(memory_space=pltpu.SMEM)] * len(table) + in_hbm,
        out_specs=pl.BlockSpec(memory_space=pltpu.VMEM),
        out_shape=jax.ShapeDtypeStruct(shape, pieces[0].dtype),
        scratch_shapes=[pltpu.SemaphoreType.DMA((n_sems,))],
        cost_estimate=pl.CostEstimate(
            flops=1 << 31, bytes_accessed=4 * shape[0] * shape[1], transcendentals=0
        ),
        compiler_params=pltpu.CompilerParams(vmem_limit_bytes=(2 * shape[0] * shape[1]) + (2 << 20)),
    )(*table, *pieces)


def gather_weight(own, size):
    half = own.shape[0] // 2
    by_far, by_row = hop(own, FAR, size), hop(own, ROW, size)
    corner_top = hop(by_far[:half], ROW, size)
    corner_low = hop(by_row[half:], FAR, size)
    mine = [own, by_row, by_far, corner_top, corner_low]
    return mine + [hop(v, NEAR, size) for v in mine]


def scatter_weight(partial_of, size, scale):
    f32 = jnp.float32
    other = hop(partial_of(True), NEAR, size)
    own = partial_of(False)

    def both(*at):
        return own[at].astype(f32) + other[at].astype(f32)

    def sent(value, mask):
        return hop(value, mask, size)

    to_far = both(slice(2, 4), 0).astype(own.dtype)
    to_row = both(slice(1, 4, 2), 1).astype(own.dtype)
    from_far = sent(to_far, FAR)
    from_row = sent(to_row, ROW)
    to_top = (both(1, 0) + from_far[1].astype(f32)).astype(own.dtype)
    to_low = (both(2, 1) + from_row[1].astype(f32)).astype(own.dtype)
    top_last = sent(to_top, ROW)
    low_last = sent(to_low, FAR)
    own, other, from_far, from_row, top_last, low_last = lax.optimization_barrier(
        (own, other, from_far, from_row, top_last, low_last)
    )
    firsts, lasts = jnp.stack([from_far[0], from_row[0]]), jnp.stack([top_last, low_last])
    total = (both(0) + firsts.astype(f32) + lasts.astype(f32)) * scale
    return total.reshape((-1, total.shape[-1]))


def hop_body(size, n_col, act_in, cot_out, w_gate, w_up, w_down):
    tok_rows = act_in.shape[0]
    rows, cols = w_gate.shape
    me = lax.axis_index(GROUP)
    place = lax.axis_index("col")
    per_col = size // n_col
    bf16, f32 = jnp.bfloat16, jnp.float32

    def dot(left, right, left_dim, right_dim):
        return lax.dot_general(
            left,
            right,
            (((left_dim,), (right_dim,)), ((), ())),
            preferred_element_type=f32,
        )

    acts = line_gather(act_in.T, size)
    cots = line_gather(cot_out.T, size)
    gate_rows = gather_weight(w_gate, size)
    up_rows = gather_weight(w_up, size)
    down_rows = gather_weight(w_down.T, size)
    k = me ^ jnp.array(MASKS, jnp.int32)
    source = jnp.stack([line_slot(k // per_col), lax.rem(k, per_col)])

    gate_all = lay_out(gate_rows, (size * rows, cols))
    up_all = lay_out(up_rows, (size * rows, cols))
    down_all = lay_out(down_rows, (size * rows, cols))
    act_t = lay_out(acts, (size * rows, tok_rows), source)
    cot_t = lay_out(cots, (size * rows, tok_rows), source)

    gate_pre = dot(act_t, gate_all, 0, 0)
    up_pre = dot(act_t, up_all, 0, 0)
    act_val, slope_val = gelu_parts(gate_pre)
    act_val, slope_up, hidden = lax.optimization_barrier(
        (act_val, slope_val * up_pre, (act_val * up_pre).astype(bf16))
    )
    hidden_grad = dot(cot_t, down_all, 0, 0)
    d_gate = (hidden_grad * slope_up).astype(bf16)
    d_up = (hidden_grad * act_val).astype(bf16)

    norm_scale = 1.0 / math.sqrt(tok_rows * size)
    own_rows = rows * len(OWN_MASKS)

    def weight_grad(left_t, right):
        def partial_of(near):
            part = left_t[own_rows:] if near else left_t[:own_rows]
            out = dot(part, right, 1, 0).astype(bf16)
            return out.reshape((len(OWN_MASKS), 2, rows // 2, -1))

        return scatter_weight(partial_of, size, norm_scale)

    down_grad = weight_grad(cot_t, hidden).T
    gate_grad = weight_grad(act_t, d_gate)
    up_grad = weight_grad(act_t, d_up)

    terms = dot(gate_all, d_gate, 1, 1) + dot(up_all, d_up, 1, 1)
    terms = terms.astype(bf16).reshape((n_col, per_col * rows, tok_rows))

    def term_of(piece):
        bits = piece ^ (me // per_col)
        return lax.dynamic_index_in_dim(terms, (bits & 1) * 2 + bits // 2, 0, keepdims=False)

    left, at_end = place < 2, (place == 0) | (place == 3)
    near_end, near_inner = jnp.where(left, 0, 3), jnp.where(left, 1, 2)
    far_end, far_inner = 3 - near_end, 3 - near_inner
    outer = [(0, 1), (1, 0), (2, 3), (3, 2)]
    beside_far = shift(term_of(jnp.where(at_end, far_end, near_end)), outer)
    beside = shift(term_of(jnp.where(at_end, far_inner, near_end)), outer)
    for_end = (term_of(far_end).astype(f32) + beside_far.astype(f32)).astype(bf16)
    over_end = middle(for_end, size)
    beside, _ = lax.optimization_barrier((beside, for_end))
    for_inner = (term_of(far_inner).astype(f32) + beside.astype(f32)).astype(bf16)
    over = middle(for_inner, size)
    back = jnp.where(at_end, term_of(near_inner), over_end)
    last = shift(back, outer)
    last, over, beside_far = lax.optimization_barrier((last, over, beside_far))
    total = term_of(place).astype(f32) + last.astype(f32)
    total = (total + jnp.where(at_end, beside_far, over).astype(f32)).astype(bf16)
    swapped = jnp.concatenate([total[rows:], total[:rows]], axis=0)
    input_grad = jnp.where((me & ROW) == 0, total, swapped).T
    return (input_grad, gate_grad, up_grad, down_grad)


def solution(mesh):
    n_dp, n_row, n_col = (mesh.shape[a] for a in ("dp", "row", "col"))
    size = n_dp * n_row
    by_tokens = P(GROUP, "col")
    hops = size == len(MASKS) and n_row == 2 and n_col == 4

    def body(*args):
        if not hops:
            return plain_body(*args)
        return hop_body(size, n_col, *args)

    return jax.shard_map(
        body,
        mesh=mesh,
        in_specs=(by_tokens,) * 4 + (P("col", GROUP),),
        out_specs=(by_tokens,) * 3 + (P("col", GROUP),),
        check_vma=False,
    )
```
